16 devices in a mesh: dp: 2 (over y, z), tp: 8 (over x, core).
Axes of the slice: x: 4, y: 2, z: 1, core: 2. Of those that a mesh axis runs over, the one named last changes fastest.
The devices are a block of a 4x4x8 slice.
Arguments:
- x_norm: bfloat16 [1024, 1536], P(('dp', 'tp')), parts along dimension 0
- w_gate: bfloat16 [1536, 8960], P(None, 'tp')
- w_up: bfloat16 [1536, 8960], P(None, 'tp')
- w_down: bfloat16 [8960, 1536], P('tp')
- u_gate: bfloat16 [1024, 8960], P('dp', 'tp'), parts along dimension 0
- u_up: bfloat16 [1024, 8960], P('dp', 'tp'), parts along dimension 0
- grad_out: bfloat16 [1024, 1536], P(('dp', 'tp')), parts along dimension 0
Outputs:
- output 1: bfloat16 [1024, 1536], P(('dp', 'tp')), parts along dimension 0
- output 2: float32 [3072, 8960], P('dp', 'tp'), parts along dimension 0
- output 3: float32 [3072, 8960], P('dp', 'tp'), parts along dimension 0
- output 4: float32 [17920, 1536], P(('dp', 'tp')), parts along dimension 0
There are 2 independent parts. The reference program is written for one: setup_inputs(seed, part) draws one part's arguments, and reference() takes and returns one part's arrays. A program takes and returns all parts, laid end to end along the dimension named above; an argument that names none is the same for every part.
All inputs are finite; a program needn't handle non-finite values.
Results may differ from the reference program's by a relative error of at most 0.0130562.
Values are sent between devices in bfloat16 or wider.
A program may use at most 768 MiB of HBM per device.

```python
import jax
import jax.numpy as jnp

TOKENS = 512
HIDDEN = 1536
FFN_DIM = 8960


def setup_inputs(seed: int = 0, part: int = 0) -> dict:
    shared_keys = jax.random.split(jax.random.key(seed + 1), 3)
    own_keys = jax.random.split(jax.random.fold_in(jax.random.key(seed), part), 4)
    x_norm = jax.random.normal(own_keys[0], (TOKENS, HIDDEN), jnp.float32)
    w_gate = jax.random.normal(shared_keys[0], (HIDDEN, FFN_DIM), jnp.float32) * HIDDEN ** -0.5
    w_up = jax.random.normal(shared_keys[1], (HIDDEN, FFN_DIM), jnp.float32) * HIDDEN ** -0.5
    w_down = jax.random.normal(shared_keys[2], (FFN_DIM, HIDDEN), jnp.float32) * FFN_DIM ** -0.5
    u_gate = jax.random.normal(own_keys[1], (TOKENS, FFN_DIM), jnp.float32)
    u_up = jax.random.normal(own_keys[2], (TOKENS, FFN_DIM), jnp.float32)
    grad_out = jax.random.normal(own_keys[3], (TOKENS, HIDDEN), jnp.float32)
    return {
        'x_norm': x_norm.astype(jnp.bfloat16),
        'w_gate': w_gate.astype(jnp.bfloat16),
        'w_up': w_up.astype(jnp.bfloat16),
        'w_down': w_down.astype(jnp.bfloat16),
        'u_gate': u_gate.astype(jnp.bfloat16),
        'u_up': u_up.astype(jnp.bfloat16),
        'grad_out': grad_out.astype(jnp.bfloat16),
    }


def reference(x_norm, w_gate, w_up, w_down, u_gate, u_up, grad_out):
    gate_pre = u_gate.astype(jnp.float32)
    up_pre = u_up.astype(jnp.float32)
    sig_gate = jax.nn.sigmoid(gate_pre)
    gate_act = gate_pre * sig_gate
    z_act = (gate_act * up_pre).astype(jnp.bfloat16)
    grad_down = jnp.dot(z_act.T, grad_out, preferred_element_type=jnp.float32)
    grad_hid = jnp.dot(grad_out, w_down.T, preferred_element_type=jnp.float32)
    grad_up = (grad_hid * gate_act).astype(jnp.bfloat16)
    silu_prime = sig_gate * (1.0 + gate_pre * (1.0 - sig_gate))
    grad_gate = (grad_hid * up_pre * silu_prime).astype(jnp.bfloat16)
    grad_x = (jnp.dot(grad_gate, w_gate.T, preferred_element_type=jnp.float32)
              + jnp.dot(grad_up, w_up.T, preferred_element_type=jnp.float32)).astype(jnp.bfloat16)
    grad_wg = jnp.dot(x_norm.T, grad_gate, preferred_element_type=jnp.float32)
    grad_wu = jnp.dot(x_norm.T, grad_up, preferred_element_type=jnp.float32)
    return (grad_x, grad_wg, grad_wu, grad_down)
```

```python
import functools

import jax
import jax.numpy as jnp
from jax import lax
from jax.experimental import pallas as pl
from jax.experimental.pallas import tpu as pltpu
from jax.sharding import PartitionSpec as P

MESH = pl.DeviceIdType.MESH
CONTRACT_ROWS = (((0,), (0,)), ((), ()))
CONTRACT_COLS = (((1,), (1,)), ((), ()))
HBM = pl.BlockSpec(memory_space=pltpu.HBM)
VMEM = pl.BlockSpec(memory_space=pltpu.VMEM)


def _tiles(total, size):
    return [(at, min(size, total - at)) for at in range(0, total, size)]


def exchange_kernel(chips, x_hbm, dy_hbm, wg_hbm, wu_hbm, wd_hbm, ug_hbm, uu_hbm,
                    dx_out, xb, dug, duu, dwd,
                    dyb, wg, wu, wd, ug, uu, act, slope, z, part, peer, summed, mid, fin,
                    load_sem, send_sem, recv_sem):
    own = dy_hbm.shape[0]
    half = own // 2
    rows = 2 * own
    hidden = dy_hbm.shape[1]
    width = ug_hbm.shape[0]
    me = lax.axis_index('tp')
    chip, core = me // 2, me % 2
    right = lax.rem(chip + 1, chips) * 2 + core
    left = lax.rem(chip + chips - 1, chips) * 2 + core
    partner = chip * 2 + 1 - core
    mine = pl.multiple_of(core * own, own)
    other = pl.multiple_of((1 - core) * own, own)

    loads = {}

    def load(name, src, dst):
        copy = pltpu.make_async_copy(src, dst, load_sem.at[len(loads)])
        copy.start()
        loads[name] = copy

    load('dy', dy_hbm, dyb.at[pl.ds(mine, own)])
    load('x', x_hbm, xb.at[pl.ds(mine, own)])
    for slot, ahead in enumerate((0, 1, chips - 1, 2)):
        at = pl.multiple_of(lax.rem(chip + ahead, chips) * rows, rows)
        load(f'ug{slot}', ug_hbm.at[:, pl.ds(at, rows)], ug.at[:, pl.ds(slot * rows, rows)])
        load(f'uu{slot}', uu_hbm.at[:, pl.ds(at, rows)], uu.at[:, pl.ds(slot * rows, rows)])
    load('wd', wd_hbm, wd)
    load('wg', wg_hbm, wg)
    load('wu', wu_hbm, wu)

    barrier = pltpu.get_barrier_semaphore()
    for device in (left, right, partner):
        pl.semaphore_signal(barrier, inc=1, device_id={'tp': device}, device_id_type=MESH)
    pl.semaphore_wait(barrier, 3)

    copies = []

    def remote(src, dst, device):
        at = len(copies)
        copy = pltpu.make_async_remote_copy(
            src_ref=src, dst_ref=dst, send_sem=send_sem.at[at], recv_sem=recv_sem.at[at],
            device_id={'tp': device}, device_id_type=MESH)
        copies.append(copy)
        copy.start()
        return copy

    def span(buf, slot, which):
        return buf.at[pl.ds(pl.multiple_of(slot * rows + mine + which * half, half), half)]

    def send_own(buf):
        full = buf.at[pl.ds(mine, own)]
        got = {}
        got['2a'] = remote(span(buf, 0, 0), span(buf, 2, 0), right)
        got['1b'] = remote(span(buf, 0, 1), span(buf, 1, 1), left)
        got['2b'] = remote(span(buf, 0, 1), span(buf, 2, 1), right)
        got['1a'] = remote(span(buf, 0, 0), span(buf, 1, 0), left)
        got['0'] = remote(full, full, partner)
        return got

    def share(buf, got, slot, which):
        key = f'{slot}{"ab"[which]}'
        got[key].wait_recv()
        piece = span(buf, slot, which)
        if key == '2a':
            got['3a'] = remote(piece, span(buf, 3, 0), right)
        if key == '1b':
            got['3b'] = remote(piece, span(buf, 3, 1), left)
        got['p' + key] = remote(piece, piece, partner)

    def gate():
        for slot in range(4):
            loads[f'ug{slot}'].wait()
            loads[f'uu{slot}'].wait()

        def body(i, _):
            at = pl.ds(pl.multiple_of(i * 32, 32), 32)
            gate_pre = ug[at, :].astype(jnp.float32)
            up_pre = uu[at, :].astype(jnp.float32)
            sig = jax.nn.sigmoid(gate_pre)
            gate_act = gate_pre * sig
            act[at, :] = gate_act
            slope[at, :] = sig * (1.0 + gate_pre * (1.0 - sig))
            z[at, :] = (gate_act * up_pre).astype(jnp.bfloat16)
            return 0

        lax.fori_loop(0, width // 32, body, 0)

    def hidden_grad(slot, count):
        at = slice(slot * rows, (slot + count) * rows)
        dy = dyb[at, :]
        for m0, m in _tiles(width, width // 2):
            f = slice(m0, m0 + m)
            g = lax.dot_general(wd[f, :], dy, CONTRACT_COLS, preferred_element_type=jnp.float32)
            duu[f, at] = (g * act[f, at]).astype(jnp.bfloat16)
            dug[f, at] = (g * uu[f, at].astype(jnp.float32) * slope[f, at]).astype(jnp.bfloat16)

    def input_grad(slot, count):
        at = slice(slot * rows, (slot + count) * rows)
        for n0, n in _tiles(hidden, hidden // 2):
            cols = slice(n0, n0 + n)
            total = (lax.dot_general(dug[:, at], wg[:, cols], CONTRACT_ROWS, preferred_element_type=jnp.float32)
                     + lax.dot_general(duu[:, at], wu[:, cols], CONTRACT_ROWS, preferred_element_type=jnp.float32))
            part[at, cols] = total.astype(jnp.bfloat16)

    def swap(slot):
        return remote(part.at[pl.ds(pl.multiple_of(slot * rows + other, own), own)],
                      peer.at[pl.ds(slot * own, own)], partner)

    def pair_sum(slot):
        a = part[pl.ds(pl.multiple_of(slot * rows + mine, own), own), :].astype(jnp.float32)
        return a + peer[slot * own:(slot + 1) * own, :].astype(jnp.float32)

    loads['dy'].wait()
    dy_got = send_own(dyb)
    gate()
    dy_got['0'].wait_recv()
    loads['wd'].wait()
    hidden_grad(0, 1)
    share(dyb, dy_got, 2, 0)
    share(dyb, dy_got, 1, 1)
    loads['x'].wait()
    x_got = send_own(xb)
    loads['wg'].wait()
    loads['wu'].wait()
    input_grad(0, 1)
    share(dyb, dy_got, 2, 1)
    share(dyb, dy_got, 1, 0)
    swaps = {0: swap(0)}
    for key in ('p2a', 'p1b', 'p2b', 'p1a'):
        dy_got[key].wait_recv()
    hidden_grad(1, 2)
    share(dyb, dy_got, 3, 0)
    share(dyb, dy_got, 3, 1)
    share(xb, x_got, 2, 0)
    share(xb, x_got, 1, 1)
    input_grad(1, 2)
    swaps[1] = swap(1)
    swaps[2] = swap(2)
    dy_got['p3a'].wait_recv()
    dy_got['p3b'].wait_recv()
    hidden_grad(3, 1)
    input_grad(3, 1)
    swaps[3] = swap(3)
    share(xb, x_got, 2, 1)
    share(xb, x_got, 1, 0)

    for slot in (1, 2):
        swaps[slot].wait_recv()
        summed[slot * own:(slot + 1) * own, :] = pair_sum(slot).astype(jnp.bfloat16)
    swaps[3].wait_recv()
    summed[3 * own:4 * own, :] = pair_sum(3).astype(jnp.bfloat16)

    def block(buf, slot, which):
        return buf.at[pl.ds(slot * own + which * half, half)]

    far_a = remote(block(summed, 3, 0), block(mid, 0, 0), right)
    far_b = remote(block(summed, 3, 1), block(mid, 0, 1), left)
    near_rb = remote(block(summed, 1, 1), block(fin, 1, 1), right)
    near_la = remote(block(summed, 2, 0), block(fin, 0, 0), left)
    swaps[0].wait_recv()
    for m0, m in _tiles(width, width // 4):
        dwd[m0:m0 + m, :] = jnp.dot(z[m0:m0 + m, :], dyb[...], preferred_element_type=jnp.float32)
    far_a.wait_recv()
    total = summed[own:own + half, :].astype(jnp.float32) + mid[:half, :].astype(jnp.float32)
    summed[0:half, :] = total.astype(jnp.bfloat16)
    near_ra = remote(block(summed, 0, 0), block(fin, 1, 0), right)
    far_b.wait_recv()
    total = summed[2 * own + half:3 * own, :].astype(jnp.float32) + mid[half:, :].astype(jnp.float32)
    summed[half:own, :] = total.astype(jnp.bfloat16)
    near_lb = remote(block(summed, 0, 1), block(fin, 0, 1), left)
    share(xb, x_got, 3, 0)
    share(xb, x_got, 3, 1)
    for copy in (near_rb, near_la, near_ra, near_lb):
        copy.wait_recv()
    dx = pair_sum(0) + fin[:own, :].astype(jnp.float32) + fin[own:, :].astype(jnp.float32)
    dx_out[...] = dx.astype(jnp.bfloat16)
    x_got['0'].wait_recv()
    for key in ('p2a', 'p1b', 'p2b', 'p1a', 'p3a', 'p3b'):
        x_got[key].wait_recv()
    for copy in copies:
        copy.wait_send()


def weight_kernel(dx, xb, dug, duu, dwd, dx_out, dwg_out, dwu_out, dwd_out, tile, sem, out_sem):
    tile_rows = tile.shape[1]
    slots = tile.shape[0]
    down = pltpu.make_async_copy(dwd, dwd_out, sem.at[0])
    down.start()
    small = pltpu.make_async_copy(dx, dx_out, sem.at[1])
    small.start()
    flying = {}
    step = 0
    for m0, m in _tiles(dug.shape[0], tile_rows):
        for grad, out in ((dug, dwg_out), (duu, dwu_out)):
            slot = step % slots
            if slot in flying:
                flying[slot].wait()
            tile[slot] = jnp.dot(grad[m0:m0 + m, :], xb[...], preferred_element_type=jnp.float32)
            copy = pltpu.make_async_copy(tile.at[slot], out.at[pl.ds(m0, m)], out_sem.at[slot])
            copy.start()
            flying[slot] = copy
            step += 1
    for copy in flying.values():
        copy.wait()
    down.wait()
    small.wait()


def solution(mesh):
    chips = mesh.shape['tp'] // 2

    def local_backward(x_loc, wg_loc, wu_loc, wd_loc, ug_loc, uu_loc, dy_loc):
        own, hidden = dy_loc.shape
        tokens, width = ug_loc.shape
        bf16, f32 = jnp.bfloat16, jnp.float32
        n_copies = 2 * (5 + 2 + 6) + 4 + 6
        dx, x_all, dug, duu, dwd = pl.pallas_call(
            functools.partial(exchange_kernel, chips),
            out_shape=[pltpu.VMEM((own, hidden), bf16),
                       pltpu.VMEM((tokens, hidden), bf16),
                       pltpu.VMEM((width, tokens), bf16),
                       pltpu.VMEM((width, tokens), bf16),
                       pltpu.VMEM((width, hidden), f32)],
            in_specs=[HBM] * 7,
            out_specs=[VMEM] * 5,
            scratch_shapes=[
                pltpu.VMEM((tokens, hidden), bf16),
                pltpu.VMEM((width, hidden), bf16),
                pltpu.VMEM((width, hidden), bf16),
                pltpu.VMEM((width, hidden), bf16),
                pltpu.VMEM((width, tokens), bf16),
                pltpu.VMEM((width, tokens), bf16),
                pltpu.VMEM((width, tokens), f32),
                pltpu.VMEM((width, tokens), f32),
                pltpu.VMEM((width, tokens), bf16),
                pltpu.VMEM((tokens, hidden), bf16),
                pltpu.VMEM((4 * own, hidden), bf16),
                pltpu.VMEM((4 * own, hidden), bf16),
                pltpu.VMEM((own, hidden), bf16),
                pltpu.VMEM((2 * own, hidden), bf16),
                pltpu.SemaphoreType.DMA((13,)),
                pltpu.SemaphoreType.DMA((n_copies,)),
                pltpu.SemaphoreType.DMA((n_copies,)),
            ],
            compiler_params=pltpu.CompilerParams(
                collective_id=0, has_side_effects=True, vmem_limit_bytes=44 * 2**20),
            name='exchange',
        )(x_loc, dy_loc, wg_loc.T, wu_loc.T, wd_loc, ug_loc.T, uu_loc.T)
        dx, dwg, dwu, dwd = pl.pallas_call(
            weight_kernel,
            out_shape=[jax.ShapeDtypeStruct((own, hidden), bf16)]
            + [jax.ShapeDtypeStruct((width, hidden), f32)] * 3,
            in_specs=[VMEM] * 5,
            out_specs=[HBM] * 4,
            scratch_shapes=[
                pltpu.VMEM((4, width // 4, hidden), f32),
                pltpu.SemaphoreType.DMA((2,)),
                pltpu.SemaphoreType.DMA((4,)),
            ],
            compiler_params=pltpu.CompilerParams(vmem_limit_bytes=24 * 2**20),
            name='weights',
        )(dx, x_all, dug, duu, dwd)
        return dx, dwg.T, dwu.T, dwd

    tok_spec = P(('dp', 'tp'), None)
    col_spec = P(None, 'tp')
    act_spec = P('dp', 'tp')
    return jax.shard_map(local_backward, mesh=mesh,
                         in_specs=(tok_spec, col_spec, col_spec, P('tp', None), act_spec, act_spec, tok_spec),
                         out_specs=(tok_spec, act_spec, act_spec, tok_spec),
                         check_vma=False)
```

```python
import functools

import jax
import jax.numpy as jnp
from jax import lax
from jax.experimental import pallas as pl
from jax.experimental.pallas import tpu as pltpu
from jax.sharding import PartitionSpec as P

MESH = pl.DeviceIdType.MESH
CONTRACT_ROWS = (((0,), (0,)), ((), ()))
CONTRACT_COLS = (((1,), (1,)), ((), ()))
HBM = pl.BlockSpec(memory_space=pltpu.HBM)
VMEM = pl.BlockSpec(memory_space=pltpu.VMEM)


def _tiles(total, size):
    return [(at, min(size, total - at)) for at in range(0, total, size)]


def exchange_kernel(chips, x_hbm, dy_hbm, wg_hbm, wu_hbm, wd_hbm, ug_hbm, uu_hbm,
                    keep, fin, xb, dug, duu, dwd,
                    dyb, wg, wu, wd, ug, uu, act, slope, z, part, peer, far, mid, near,
                    load_sem, send_sem, recv_sem):
    own = dy_hbm.shape[0]
    half = own // 2
    rows = 2 * own
    hidden = dy_hbm.shape[1]
    width = ug_hbm.shape[0]
    me = lax.axis_index('tp')
    chip, core = me // 2, me % 2
    right = lax.rem(chip + 1, chips) * 2 + core
    left = lax.rem(chip + chips - 1, chips) * 2 + core
    partner = chip * 2 + 1 - core
    mine = pl.multiple_of(core * own, own)
    other = pl.multiple_of((1 - core) * own, own)

    loads = {}

    def load(name, src, dst):
        copy = pltpu.make_async_copy(src, dst, load_sem.at[len(loads)])
        copy.start()
        loads[name] = copy

    load('dy', dy_hbm, dyb.at[pl.ds(mine, own)])
    load('x', x_hbm, xb.at[pl.ds(mine, own)])
    for slot, ahead in enumerate((0, 1, chips - 1, 2)):
        at = pl.multiple_of(lax.rem(chip + ahead, chips) * rows, rows)
        load(f'ug{slot}', ug_hbm.at[:, pl.ds(at, rows)], ug.at[:, pl.ds(slot * rows, rows)])
        load(f'uu{slot}', uu_hbm.at[:, pl.ds(at, rows)], uu.at[:, pl.ds(slot * rows, rows)])
    load('wd', wd_hbm, wd)
    load('wg', wg_hbm, wg)
    load('wu', wu_hbm, wu)

    barrier = pltpu.get_barrier_semaphore()
    for device in (left, right, partner):
        pl.semaphore_signal(barrier, inc=1, device_id={'tp': device}, device_id_type=MESH)
    pl.semaphore_wait(barrier, 3)

    copies = []

    def remote(src, dst, device):
        at = len(copies)
        copy = pltpu.make_async_remote_copy(
            src_ref=src, dst_ref=dst, send_sem=send_sem.at[at], recv_sem=recv_sem.at[at],
            device_id={'tp': device}, device_id_type=MESH)
        copies.append(copy)
        copy.start()
        return copy

    def span(buf, slot, which):
        return buf.at[pl.ds(pl.multiple_of(slot * rows + mine + which * half, half), half)]

    def send_first(buf):
        full = buf.at[pl.ds(mine, own)]
        return {'2a': remote(span(buf, 0, 0), span(buf, 2, 0), right),
                '1b': remote(span(buf, 0, 1), span(buf, 1, 1), left),
                '0': remote(full, full, partner)}

    def send_second(buf, got):
        got['2b'] = remote(span(buf, 0, 1), span(buf, 2, 1), right)
        got['1a'] = remote(span(buf, 0, 0), span(buf, 1, 0), left)

    def share(buf, got, slot, which):
        key = f'{slot}{"ab"[which]}'
        got[key].wait_recv()
        piece = span(buf, slot, which)
        if key == '2a':
            got['3a'] = remote(piece, span(buf, 3, 0), right)
        if key == '1b':
            got['3b'] = remote(piece, span(buf, 3, 1), left)
        got['p' + key] = remote(piece, piece, partner)

    def gate(first, last):
        def body(i, _):
            at = pl.ds(pl.multiple_of(i * 32, 32), 32)
            gate_pre = ug[at, :].astype(jnp.float32)
            up_pre = uu[at, :].astype(jnp.float32)
            sig = jax.nn.sigmoid(gate_pre)
            gate_act = gate_pre * sig
            act[at, :] = gate_act
            slope[at, :] = sig * (1.0 + gate_pre * (1.0 - sig))
            z[at, :] = (gate_act * up_pre).astype(jnp.bfloat16)
            return 0

        lax.fori_loop(first, last, body, 0)

    def hidden_grad(slot, count):
        at = slice(slot * rows, (slot + count) * rows)
        dy = dyb[at, :]
        for m0, m in _tiles(width, width // 2):
            f = slice(m0, m0 + m)
            g = lax.dot_general(wd[f, :], dy, CONTRACT_COLS, preferred_element_type=jnp.float32)
            duu[f, at] = (g * act[f, at]).astype(jnp.bfloat16)
            dug[f, at] = (g * uu[f, at].astype(jnp.float32) * slope[f, at]).astype(jnp.bfloat16)

    def input_grad(slot, count):
        at = slice(slot * rows, (slot + count) * rows)
        for n0, n in _tiles(hidden, hidden // 2):
            cols = slice(n0, n0 + n)
            total = (lax.dot_general(dug[:, at], wg[:, cols], CONTRACT_ROWS, preferred_element_type=jnp.float32)
                     + lax.dot_general(duu[:, at], wu[:, cols], CONTRACT_ROWS, preferred_element_type=jnp.float32))
            part[at, cols] = total.astype(jnp.bfloat16)

    def swap(slot):
        return remote(part.at[pl.ds(pl.multiple_of(slot * rows + other, own), own)],
                      peer.at[pl.ds(slot * own, own)], partner)

    def pair_sum(slot):
        a = part[pl.ds(pl.multiple_of(slot * rows + mine, own), own), :].astype(jnp.float32)
        return a + peer[slot * own:(slot + 1) * own, :].astype(jnp.float32)

    def down_grad(index):
        m = width // 4
        at = slice(index * m, (index + 1) * m)
        dwd[at, :] = jnp.dot(z[at, :], dyb[...], preferred_element_type=jnp.float32)

    loads['dy'].wait()
    dy_got = send_first(dyb)
    for slot in range(4):
        loads[f'ug{slot}'].wait()
        loads[f'uu{slot}'].wait()
    steps = width // 32
    gate(0, steps // 2)
    send_second(dyb, dy_got)
    gate(steps // 2, steps)
    dy_got['0'].wait_recv()
    loads['wd'].wait()
    hidden_grad(0, 1)
    share(dyb, dy_got, 2, 0)
    share(dyb, dy_got, 1, 1)
    loads['wg'].wait()
    loads['wu'].wait()
    input_grad(0, 1)
    swaps = {0: swap(0)}
    share(dyb, dy_got, 2, 1)
    share(dyb, dy_got, 1, 0)
    loads['x'].wait()
    x_got = send_first(xb)
    for key in ('p2a', 'p1b', 'p2b', 'p1a'):
        dy_got[key].wait_recv()
    hidden_grad(1, 2)
    share(dyb, dy_got, 3, 0)
    share(dyb, dy_got, 3, 1)
    send_second(xb, x_got)
    input_grad(1, 1)
    swaps[1] = swap(1)
    dy_got['p3a'].wait_recv()
    dy_got['p3b'].wait_recv()
    hidden_grad(3, 1)
    share(xb, x_got, 2, 0)
    share(xb, x_got, 1, 1)
    input_grad(3, 1)
    swaps[3] = swap(3)
    input_grad(2, 1)
    swaps[2] = swap(2)

    def block(buf, index, which):
        return buf.at[pl.ds(index * own + which * half, half)]

    swaps[3].wait_recv()
    far[...] = pair_sum(3).astype(jnp.bfloat16)
    far_a = remote(block(far, 0, 0), block(mid, 0, 0), right)
    far_b = remote(block(far, 0, 1), block(mid, 0, 1), left)
    share(xb, x_got, 2, 1)
    share(xb, x_got, 1, 0)
    down_grad(0)
    down_grad(1)
    swaps[1].wait_recv()
    swaps[2].wait_recv()
    near_r, near_l = pair_sum(1), pair_sum(2)
    near[half:own, :] = near_r[half:].astype(jnp.bfloat16)
    near[own:own + half, :] = near_l[:half].astype(jnp.bfloat16)
    last = [remote(block(near, 0, 1), block(fin, 1, 1), right),
            remote(block(near, 1, 0), block(fin, 0, 0), left)]
    down_grad(2)
    down_grad(3)
    share(xb, x_got, 3, 0)
    share(xb, x_got, 3, 1)
    far_a.wait_recv()
    near[:half, :] = (near_r[:half] + mid[:half, :].astype(jnp.float32)).astype(jnp.bfloat16)
    last.append(remote(block(near, 0, 0), block(fin, 1, 0), right))
    far_b.wait_recv()
    near[own + half:, :] = (near_l[half:] + mid[half:, :].astype(jnp.float32)).astype(jnp.bfloat16)
    last.append(remote(block(near, 1, 1), block(fin, 0, 1), left))
    swaps[0].wait_recv()
    keep[...] = pair_sum(0)
    for key in ('0', 'p2a', 'p1b', 'p2b', 'p1a', 'p3a', 'p3b'):
        x_got[key].wait_recv()
    for copy in last:
        copy.wait_recv()
    for copy in copies:
        copy.wait_send()


def weight_kernel(keep, fin, xb, dug, duu, dwd, dx_out, dwg_out, dwu_out, dwd_out, dx, tile, sem, out_sem):
    own = keep.shape[0]
    tile_rows = tile.shape[1]
    slots = tile.shape[0]
    down = pltpu.make_async_copy(dwd, dwd_out, sem.at[0])
    down.start()
    flying = {}
    step = 0
    for m0, m in _tiles(dug.shape[0], tile_rows):
        for grad, out in ((dug, dwg_out), (duu, dwu_out)):
            slot = step % slots
            if slot in flying:
                flying[slot].wait()
            tile[slot] = jnp.dot(grad[m0:m0 + m, :], xb[...], preferred_element_type=jnp.float32)
            copy = pltpu.make_async_copy(tile.at[slot], out.at[pl.ds(m0, m)], out_sem.at[slot])
            copy.start()
            flying[slot] = copy
            step += 1
            if step == 2:
                total = keep[...] + fin[:own, :].astype(jnp.float32) + fin[own:, :].astype(jnp.float32)
                dx[...] = total.astype(jnp.bfloat16)
                small = pltpu.make_async_copy(dx, dx_out, sem.at[1])
                small.start()
    for copy in flying.values():
        copy.wait()
    down.wait()
    small.wait()


def solution(mesh):
    chips = mesh.shape['tp'] // 2

    def local_backward(x_loc, wg_loc, wu_loc, wd_loc, ug_loc, uu_loc, dy_loc):
        own, hidden = dy_loc.shape
        tokens, width = ug_loc.shape
        bf16, f32 = jnp.bfloat16, jnp.float32
        n_copies = 2 * (5 + 2 + 6) + 4 + 6
        keep, fin, x_all, dug, duu, dwd = pl.pallas_call(
            functools.partial(exchange_kernel, chips),
            out_shape=[pltpu.VMEM((own, hidden), f32),
                       pltpu.VMEM((2 * own, hidden), bf16),
                       pltpu.VMEM((tokens, hidden), bf16),
                       pltpu.VMEM((width, tokens), bf16),
                       pltpu.VMEM((width, tokens), bf16),
                       pltpu.VMEM((width, hidden), f32)],
            in_specs=[HBM] * 7,
            out_specs=[VMEM] * 6,
            scratch_shapes=[
                pltpu.VMEM((tokens, hidden), bf16),
                pltpu.VMEM((width, hidden), bf16),
                pltpu.VMEM((width, hidden), bf16),
                pltpu.VMEM((width, hidden), bf16),
                pltpu.VMEM((width, tokens), bf16),
                pltpu.VMEM((width, tokens), bf16),
                pltpu.VMEM((width, tokens), f32),
                pltpu.VMEM((width, tokens), f32),
                pltpu.VMEM((width, tokens), bf16),
                pltpu.VMEM((tokens, hidden), bf16),
                pltpu.VMEM((4 * own, hidden), bf16),
                pltpu.VMEM((own, hidden), bf16),
                pltpu.VMEM((own, hidden), bf16),
                pltpu.VMEM((2 * own, hidden), bf16),
                pltpu.SemaphoreType.DMA((13,)),
                pltpu.SemaphoreType.DMA((n_copies,)),
                pltpu.SemaphoreType.DMA((n_copies,)),
            ],
            compiler_params=pltpu.CompilerParams(
                collective_id=0, has_side_effects=True, vmem_limit_bytes=44 * 2**20),
            name='exchange',
        )(x_loc, dy_loc, wg_loc.T, wu_loc.T, wd_loc, ug_loc.T, uu_loc.T)
        dx, dwg, dwu, dwd = pl.pallas_call(
            weight_kernel,
            out_shape=[jax.ShapeDtypeStruct((own, hidden), bf16)]
            + [jax.ShapeDtypeStruct((width, hidden), f32)] * 3,
            in_specs=[VMEM] * 6,
            out_specs=[HBM] * 4,
            scratch_shapes=[
                pltpu.VMEM((own, hidden), bf16),
                pltpu.VMEM((4, width // 4, hidden), f32),
                pltpu.SemaphoreType.DMA((2,)),
                pltpu.SemaphoreType.DMA((4,)),
            ],
            compiler_params=pltpu.CompilerParams(vmem_limit_bytes=24 * 2**20),
            name='weights',
        )(keep, fin, x_all, dug, duu, dwd)
        return dx, dwg.T, dwu.T, dwd

    tok_spec = P(('dp', 'tp'), None)
    col_spec = P(None, 'tp')
    act_spec = P('dp', 'tp')
    return jax.shard_map(local_backward, mesh=mesh,
                         in_specs=(tok_spec, col_spec, col_spec, P('tp', None), act_spec, act_spec, tok_spec),
                         out_specs=(tok_spec, act_spec, act_spec, tok_spec),
                         check_vma=False)
```
